512 devices in a mesh: image: 16 (over z, x_hi), space: 32 (over y, x_lo, core).
Axes of the slice: x: 4 (x_hi: 2, x_lo: 2; x = x_hi * 2 + x_lo), y: 8, z: 8, core: 2. Of those that a mesh axis runs over, the one named last changes fastest.
Arguments:
- field: float32 [16, 128, 256, 512], P('image', 'space'), may hold values from -2.5 to 2.5
- mobility: float32 [128, 256, 512], P('space'), may hold values from 0.2 to 1
- fractions: float32 [16], P('image'), may hold values from 0.3 to 0.5
- sides: int32 [16], P('image'), may hold values from 0 to 1, as said below
Outputs:
- blended: float32 [16, 128, 256, 512], P('image', 'space')
The draws below stay inside these ranges and needn't reach their ends.
Inputs may be any that keep to these rules, and one draw needn't show every extreme that they name: `sides`: the first image always names the next one (1), the last image the previous one (0); the others name either.
All inputs are finite; a program needn't handle non-finite values.
Results may differ from the reference program's by a relative error of at most 0.00002.
Values sent between devices are 32-bit elements; how exact they have to be, the bound alone decides.
A program may use at most 128 MiB of HBM per device.

```python
import math
import jax
import jax.numpy as jnp

NY = 256
NZ = 512
STEPS = 4
NX = 128
IMAGES = 16


def draw_sides(key, part):
    values = jax.random.randint(jax.random.fold_in(key, 7), (IMAGES,), 0, 2).astype(jnp.int32)
    values = values.at[0].set(1)
    values = values.at[IMAGES - 1].set(0)
    return values


def block_levels(key, extent, cuts, least, high):
    factor_of = 1.0
    for position, blocks in cuts:
        heights = jax.random.uniform(jax.random.fold_in(jax.random.fold_in(key, 6), position), (blocks,), jnp.float32, least / len(cuts), high / len(cuts))
        factor_of = factor_of * jnp.repeat(jnp.exp(heights), extent[position] // blocks).reshape((-1,) + (1,) * (len(extent) - 1 - position))
    return factor_of


def gaussian(key, extent, spread, reach, cuts=(), kind=jnp.bfloat16):
    entries = jax.random.normal(key, extent, jnp.float32) * spread
    if len(cuts) > 0:
        entries = block_levels(key, extent, cuts, -0.22, 0.18) * entries
    return jnp.clip(entries, min=-reach, max=reach).astype(kind)


def setup_inputs(seed: int = 0) -> dict:
    keys = jax.random.split(jax.random.key(seed), 5)
    return {
        "field": gaussian(keys[0], (IMAGES, NX, NY, NZ), 0.7, 2.5, ((0, 16), (1, 32)), jnp.float32),
        "mobility": jnp.clip(jnp.exp(math.log(1.0) - 1.609438 * jax.random.uniform(keys[1], (NX, NY, NZ), jnp.float32) ** block_levels(keys[1], (NX, NY, NZ), ((0, 32),), -0.2, 0.2)), 0.2, 1.0),
        "fractions": jnp.clip(0.3 + 0.19999999 * jax.random.uniform(keys[2], (IMAGES,), jnp.float32) ** block_levels(keys[2], (IMAGES,), ((0, 16),), -0.2, 0.2), 0.3, 0.5),
        "sides": draw_sides(jax.random.fold_in(keys[4], 71), 0),
    }


DT = 0.1
EPS2 = 1.5


def advance(phi, xpad, mob):
    padded = jnp.pad(xpad, ((0, 0), (1, 1), (1, 1)))
    beside = padded[2:, 1:-1, 1:-1] + padded[:-2, 1:-1, 1:-1]
    beside = beside + padded[1:-1, 2:, 1:-1] + padded[1:-1, :-2, 1:-1]
    beside = beside + padded[1:-1, 1:-1, 2:] + padded[1:-1, 1:-1, :-2]
    return phi + DT * mob * (EPS2 * (beside - 6.0 * phi) + phi - phi * phi * phi)


def relax(phi, mobility):
    for step in range(STEPS):
        phi = advance(phi, jnp.pad(phi, ((1, 1), (0, 0), (0, 0))), mobility)
    return phi


def reference(field, mobility, fractions, sides):
    relaxed = jnp.stack([relax(field[i], mobility) for i in range(IMAGES)])
    empty = jnp.zeros_like(relaxed[:1])
    upper = jnp.concatenate([relaxed[1:], empty], axis=0)
    lower = jnp.concatenate([empty, relaxed[:-1]], axis=0)
    neighbour = jnp.where((sides == 1)[:, None, None, None], upper, lower)
    return relaxed + fractions[:, None, None, None] * (neighbour - relaxed)
```

```python
import functools

import jax
import jax.numpy as jnp
from jax import lax
from jax.experimental import pallas as pl
from jax.experimental.pallas import tpu as pltpu
from jax.sharding import PartitionSpec as P

STEPS = 4
DT = 0.1
EPS2 = 1.5
PAD = 8


def kernel(
    cfg, field, mobility, frac, sides, out,
    phi, mob, xbuf, zbuf, obuf,
    load_sem, hs, hr, xs, xr, zs, zr, osem,
):
    images, spaces, planes, ny, nz, nc = cfg
    rows = ny // nc
    img = lax.axis_index("image")
    sp = lax.axis_index("space")
    hi = lax.rem(img, 2)
    partner = img + 1 - 2 * hi
    z_to = img + 2 - 4 * hi
    z_from = img - 2 + 4 * hi
    has_l = sp > 0
    has_r = sp < spaces - 1
    has_to = jnp.logical_and(z_to >= 0, z_to < images)
    has_from = jnp.logical_and(z_from >= 0, z_from < images)
    first, last = 1, planes

    def own(t, p, c):
        return phi.at[t, p, pl.ds(PAD + pl.multiple_of(c * rows, 8), rows)]

    def seg(ref, p, c):
        return ref.at[p, pl.ds(pl.multiple_of(c * rows, 8), rows)]

    def halo(t, side, c):
        return pltpu.make_async_remote_copy(
            src_ref=own(t, last if side == 0 else first, c),
            dst_ref=own(t, 0 if side == 0 else planes + 1, c),
            send_sem=hs.at[t, side, c],
            recv_sem=hr.at[t, side, c],
            device_id={"space": sp + 1 if side == 0 else sp - 1},
            device_id_type=pl.DeviceIdType.MESH,
        )

    def xcopy(p, c):
        return pltpu.make_async_remote_copy(
            src_ref=own(STEPS, p + 1, c),
            dst_ref=seg(xbuf, p, c),
            send_sem=xs.at[p, c],
            recv_sem=xr.at[p, c],
            device_id={"image": partner},
            device_id_type=pl.DeviceIdType.MESH,
        )

    def zcopy(p, c):
        return pltpu.make_async_remote_copy(
            src_ref=seg(xbuf, p, c),
            dst_ref=seg(zbuf, p, c),
            send_sem=zs.at[p, c],
            recv_sem=zr.at[p, c],
            device_id={"image": z_to},
            device_id_type=pl.DeviceIdType.MESH,
        )

    def ocopy(p, c):
        return pltpu.make_async_copy(seg(obuf, p, c), seg(out.at[0], p, c), osem.at[p, c])

    def send_halo(t, c):
        @pl.when(has_r)
        def _():
            halo(t, 0, c).start()

        @pl.when(has_l)
        def _():
            halo(t, 1, c).start()

    def wait_halo(t, c):
        @pl.when(has_l)
        def _():
            halo(t, 0, c).wait_recv()

        @pl.when(has_r)
        def _():
            halo(t, 1, c).wait_recv()

    lane = lax.broadcasted_iota(jnp.int32, (rows, nz), 1)

    def advance(t, p, c):
        r0 = PAD + pl.multiple_of(c * rows, 8)
        here = phi[t, p, pl.ds(r0, rows)]
        s = phi[t, p - 1, pl.ds(r0, rows)] + phi[t, p + 1, pl.ds(r0, rows)]
        wide = phi[t, p, pl.ds(r0 - 8, rows + 16)]
        s = s + wide[7 : 7 + rows] + wide[9 : 9 + rows]
        s = s + jnp.where(lane == 0, 0.0, pltpu.roll(here, 1, 1))
        s = s + jnp.where(lane == nz - 1, 0.0, pltpu.roll(here, nz - 1, 1))
        m = mob[p - 1, pl.ds(pl.multiple_of(c * rows, 8), rows)]
        phi[t + 1, p, pl.ds(r0, rows)] = here + m * (EPS2 * s - here * (8.0 + here * here))

    loads = [pltpu.make_async_copy(field.at[0, p], phi.at[0, p + 1, pl.ds(PAD, ny)], load_sem.at[p]) for p in range(planes)]
    loads.append(pltpu.make_async_copy(mobility, mob, load_sem.at[planes]))
    for copy in (loads[0], loads[planes - 1], *loads[1 : planes - 1], loads[planes]):
        copy.start()

    barrier = pltpu.get_barrier_semaphore()

    def greet(axis, where, known):
        @pl.when(known)
        def _():
            pl.semaphore_signal(barrier, 1, device_id={axis: where}, device_id_type=pl.DeviceIdType.MESH)

    greet("space", sp + 1, has_r)
    greet("space", sp - 1, has_l)
    pl.semaphore_signal(barrier, 1, device_id={"image": partner}, device_id_type=pl.DeviceIdType.MESH)
    greet("image", z_to, has_to)
    greet("image", z_from, has_from)

    def clear_rows(t, _):
        for p in range(1, planes + 1):
            phi[t, p, pl.ds(0, PAD)] = jnp.zeros((PAD, nz), jnp.float32)
            phi[t, p, pl.ds(PAD + ny, PAD)] = jnp.zeros((PAD, nz), jnp.float32)
        return 0

    lax.fori_loop(0, STEPS, clear_rows, 0)

    def clear_halo(plane):
        def body(i, _):
            phi[i // nc, plane, pl.ds(PAD + pl.multiple_of(lax.rem(i, nc) * rows, 8), rows)] = jnp.zeros((rows, nz), jnp.float32)
            return 0

        lax.fori_loop(0, STEPS * nc, body, 0)

    @pl.when(jnp.logical_not(has_l))
    def _():
        clear_halo(0)

    @pl.when(jnp.logical_not(has_r))
    def _():
        clear_halo(planes + 1)

    @pl.when(jnp.logical_not(has_from))
    def _():
        def body(i, _):
            zbuf[i // nc, pl.ds(pl.multiple_of(lax.rem(i, nc) * rows, 8), rows)] = jnp.zeros((rows, nz), jnp.float32)
            return 0

        lax.fori_loop(0, planes * nc, body, 0)

    loads[0].wait()
    loads[planes - 1].wait()
    one = lambda flag: jnp.where(flag, 1, 0)
    pl.semaphore_wait(barrier, 1 + one(has_l) + one(has_r) + one(has_to) + one(has_from))

    for c in range(nc):
        send_halo(0, c)
    for p in range(1, planes - 1):
        loads[p].wait()
    loads[planes].wait()

    def scale(i, _):
        at = (i // nc, pl.ds(pl.multiple_of(lax.rem(i, nc) * rows, 8), rows))
        mob[at] = DT * mob[at]
        return 0

    lax.fori_loop(0, planes * nc, scale, 0)

    def chunk(i, _):
        t, c = i // nc, lax.rem(i, nc)
        wait_halo(t, c)
        advance(t, first, c)
        advance(t, last, c)
        for p in range(first + 1, last):
            advance(t, p, c)
        send_halo(t + 1, c)
        return 0

    lax.fori_loop(0, (STEPS - 1) * nc, chunk, 0)

    end = STEPS - 1

    def inner(c, _):
        for p in range(first + 1, last):
            advance(end, p, c)
        for p in range(first + 1, last):
            xcopy(p - 1, c).start()
        return 0

    lax.fori_loop(0, nc, inner, 0)

    def outer(c, _):
        wait_halo(end, c)
        advance(end, first, c)
        advance(end, last, c)
        xcopy(first - 1, c).start()
        xcopy(last - 1, c).start()
        return 0

    lax.fori_loop(0, nc, outer, 0)

    f = frac[0]
    use_x = sides[0] != hi
    lag = 3
    units = planes * nc

    def unit(u):
        half = u // (2 * nc)
        v = lax.rem(u, 2 * nc)
        odd = lax.rem(v, 2)
        p = jnp.where(half == 0, 1 + odd, 3 * odd)
        return p, v // 2

    def relay(u, _):
        @pl.when(u < units)
        def _():
            p, c = unit(u)
            xcopy(p, c).wait_recv()

            @pl.when(has_to)
            def _():
                zcopy(p, c).start()

        @pl.when(u >= lag)
        def _():
            p, c = unit(u - lag)

            @pl.when(has_from)
            def _():
                zcopy(p, c).wait_recv()

            at = (p, pl.ds(pl.multiple_of(c * rows, 8), rows))
            mine = phi[STEPS, p + 1, pl.ds(PAD + pl.multiple_of(c * rows, 8), rows)]
            other = jnp.where(use_x, xbuf[at], zbuf[at])
            obuf[at] = mine + f * (other - mine)
            ocopy(p, c).start()

        return 0

    lax.fori_loop(0, units + lag, relay, 0)

    def drain_halo(i, _):
        t, c = i // nc, lax.rem(i, nc)

        @pl.when(has_r)
        def _():
            halo(t, 0, c).wait_send()

        @pl.when(has_l)
        def _():
            halo(t, 1, c).wait_send()

        return 0

    lax.fori_loop(0, STEPS * nc, drain_halo, 0)

    def drain(i, _):
        p, c = i // nc, lax.rem(i, nc)
        xcopy(p, c).wait_send()

        @pl.when(has_to)
        def _():
            zcopy(p, c).wait_send()

        ocopy(p, c).wait()
        return 0

    lax.fori_loop(0, units, drain, 0)


def local(images, spaces, field, mobility, fractions, sides):
    _, planes, ny, nz = field.shape
    nc = 4
    cfg = (images, spaces, planes, ny, nz, nc)
    dma = pltpu.SemaphoreType.DMA
    return pl.pallas_call(
        functools.partial(kernel, cfg),
        out_shape=jax.ShapeDtypeStruct(field.shape, jnp.float32),
        in_specs=[
            pl.BlockSpec(memory_space=pl.ANY),
            pl.BlockSpec(memory_space=pl.ANY),
            pl.BlockSpec(memory_space=pltpu.SMEM),
            pl.BlockSpec(memory_space=pltpu.SMEM),
        ],
        out_specs=pl.BlockSpec(memory_space=pl.ANY),
        scratch_shapes=[
            pltpu.VMEM((STEPS + 1, planes + 2, ny + 2 * PAD, nz), jnp.float32),
            pltpu.VMEM((planes, ny, nz), jnp.float32),
            pltpu.VMEM((planes, ny, nz), jnp.float32),
            pltpu.VMEM((planes, ny, nz), jnp.float32),
            pltpu.VMEM((planes, ny, nz), jnp.float32),
            dma((planes + 1,)),
            dma((STEPS, 2, nc)),
            dma((STEPS, 2, nc)),
            dma((planes, nc)),
            dma((planes, nc)),
            dma((planes, nc)),
            dma((planes, nc)),
            dma((planes, nc)),
        ],
        compiler_params=pltpu.CompilerParams(
            collective_id=0, has_side_effects=True, vmem_limit_bytes=48 * 1024 * 1024
        ),
    )(field, mobility, fractions, sides)


def solution(mesh):
    return jax.shard_map(
        functools.partial(local, mesh.shape["image"], mesh.shape["space"]),
        mesh=mesh,
        in_specs=(P("image", "space", None, None), P("space", None, None), P("image"), P("image")),
        out_specs=P("image", "space", None, None),
        check_vma=False,
    )
```

```python
import functools

import jax
import jax.numpy as jnp
from jax import lax
from jax.experimental import pallas as pl
from jax.experimental.pallas import tpu as pltpu
from jax.sharding import PartitionSpec as P

STEPS = 4
DT = 0.1
EPS2 = 1.5
PAD = 8
EXT = 8
RUN = 4


def kernel(
    cfg, field, mobility, frac, sides, out,
    phi, mob, zbuf, xbuf, coef,
    ls, cs, cr, h0s, h0r, hs, hr, fs, fr, zs, zr, xs, xr,
):
    images, spaces, planes, ny, nz = cfg
    half = ny // 2
    rows = half + EXT
    unit = half // 2
    chunks = ((0, unit), (unit, rows - unit))
    parts = ((0, unit + 8), (unit + 8, rows - unit - 8))
    first, last = 1, planes
    img = lax.axis_index("image")
    sp = lax.axis_index("space")
    hi = lax.rem(img, 2)
    other = 1 - hi
    z = img // 2
    partner = img + 1 - 2 * hi
    core = lax.rem(sp, 2)
    place = lax.rem(sp, RUN)

    def half_of(which, where):
        return lax.rem(which + lax.rem(where // RUN, 2), 2)

    def base_of(h):
        return pl.multiple_of(h * (half - EXT), 8)

    h = half_of(hi, sp)
    has_l = sp > 0
    has_r = sp < spaces - 1
    in_l = core == 1
    in_r = core == 0
    img_l = 2 * z + jnp.where(place == 0, other, hi)
    img_r = 2 * z + jnp.where(place == RUN - 1, other, hi)
    has_dn = z > 0
    has_up = img < images - 2
    mesh_id = pl.DeviceIdType.MESH

    def cells(t, a, p, r, n):
        return phi.at[t, a, p, pl.ds(PAD + r, n)]

    def edge(side):
        return (last, 0, sp + 1) if side == 0 else (first, planes + 1, sp - 1)

    def halo0(side, tgt):
        p, q, where = edge(side)
        return pltpu.make_async_remote_copy(
            src_ref=field.at[0, p - 1, pl.ds(base_of(half_of(tgt, where)), rows)],
            dst_ref=cells(0, hi, q, 0, rows),
            send_sem=h0s.at[side, tgt],
            recv_sem=h0r.at[side, hi],
            device_id={"image": 2 * z + tgt, "space": where},
            device_id_type=mesh_id,
        )

    def halo_in(side, a):
        p, q, where = edge(side)
        return pltpu.make_async_remote_copy(
            src_ref=cells(0, a, p, 0, rows),
            dst_ref=cells(0, a, q, 0, rows),
            send_sem=h0s.at[side, a],
            recv_sem=h0r.at[side, a],
            device_id={"image": img, "space": where},
            device_id_type=mesh_id,
        )

    def halo(t, side, a, c):
        p, q, where = edge(side)
        r, n = chunks[c]
        return pltpu.make_async_remote_copy(
            src_ref=cells(t, a, p, r, n),
            dst_ref=cells(t, a, q, r, n),
            send_sem=hs.at[t - 1, side, a, c],
            recv_sem=hr.at[t - 1, side, a, c],
            device_id={"image": img_r if side == 0 else img_l, "space": where},
            device_id_type=mesh_id,
        )

    def fcopy(i, p, a):
        r, n = parts[i]
        return pltpu.make_async_remote_copy(
            src_ref=field.at[0, p, pl.ds(base_of(1 - h) + r, n)],
            dst_ref=cells(0, a, p + 1, r, n),
            send_sem=fs.at[i, p],
            recv_sem=fr.at[i, p],
            device_id={"image": partner},
            device_id_type=mesh_id,
        )

    def rows_of(ref, k, p, c):
        return ref.at[k, p, pl.ds(pl.multiple_of(c * unit, 8), unit)]

    def zcopy(a, p, c):
        return pltpu.make_async_remote_copy(
            src_ref=cells(STEPS, a, p + 1, pl.multiple_of(h * EXT + c * unit, 8), unit),
            dst_ref=rows_of(zbuf, 1 - a, p, c),
            send_sem=zs.at[a, p, c],
            recv_sem=zr.at[1 - a, p, c],
            device_id={"image": img - 2 + 4 * a},
            device_id_type=mesh_id,
        )

    def xcopy(p, c, which):
        return pltpu.make_async_remote_copy(
            src_ref=xbuf.at[p, pl.ds(pl.multiple_of(c * unit, 8), unit)],
            dst_ref=out.at[0, p, pl.ds(pl.multiple_of(which * half + c * unit, 8), unit)],
            send_sem=xs.at[p, c],
            recv_sem=xr.at[p, c],
            device_id={"image": partner},
            device_id_type=mesh_id,
        )

    def ccopy(a):
        return pltpu.make_async_remote_copy(
            src_ref=coef.at[a],
            dst_ref=coef.at[a],
            send_sem=cs,
            recv_sem=cr,
            device_id={"image": partner},
            device_id_type=mesh_id,
        )

    def when(flag, *more):
        for item in more:
            flag = jnp.logical_and(flag, item)
        return pl.when(flag)

    def send_halo(t, a, c):
        @when(has_r)
        def _():
            halo(t, 0, a, c).start()

        @when(has_l)
        def _():
            halo(t, 1, a, c).start()

    def wait_halo(t, a, c):
        @when(has_l)
        def _():
            halo(t, 0, a, c).wait_recv()

        @when(has_r)
        def _():
            halo(t, 1, a, c).wait_recv()

    def advance(t, a, p, c):
        r, n = chunks[c]
        lane = lax.broadcasted_iota(jnp.int32, (n, nz), 1)
        here = phi[t, a, p, pl.ds(PAD + r, n)]
        s = phi[t, a, p - 1, pl.ds(PAD + r, n)] + phi[t, a, p + 1, pl.ds(PAD + r, n)]
        wide = phi[t, a, p, pl.ds(PAD + r - 8, n + 16)]
        s = s + wide[7 : 7 + n] + wide[9 : 9 + n]
        s = s + jnp.where(lane == 0, 0.0, pltpu.roll(here, 1, 1))
        s = s + jnp.where(lane == nz - 1, 0.0, pltpu.roll(here, nz - 1, 1))
        m = mob[p - 1, pl.ds(r, n)]
        phi[t + 1, a, p, pl.ds(PAD + r, n)] = here + m * (EPS2 * s - here * (8.0 + here * here))

    inner = tuple(range(first + 1, last))

    loads = [
        pltpu.make_async_copy(field.at[0, p, pl.ds(base_of(h), rows)], cells(0, hi, p + 1, 0, rows), ls.at[p])
        for p in range(planes)
    ]
    loads.append(pltpu.make_async_copy(mobility.at[pl.ds(0, planes), pl.ds(base_of(h), rows)], mob, ls.at[planes]))
    for copy in loads:
        copy.start()

    barrier = pltpu.get_barrier_semaphore()

    def greet(where_img, where_sp):
        pl.semaphore_signal(barrier, 1, device_id={"image": where_img, "space": where_sp}, device_id_type=mesh_id)

    for side, known, inside in ((1, has_l, in_l), (0, has_r, in_r)):
        where = edge(side)[2]

        @when(known, inside)
        def _():
            greet(img, where)

        @when(known, jnp.logical_not(inside))
        def _():
            greet(2 * z, where)
            greet(2 * z + 1, where)

    greet(partner, sp)

    @when(has_dn)
    def _():
        greet(img - 2, sp)

    @when(has_up)
    def _():
        greet(img + 2, sp)

    coef[hi, 0] = jnp.full((8, nz), frac[0], jnp.float32)
    coef[hi, 1] = jnp.full((8, nz), sides[0].astype(jnp.float32), jnp.float32)

    def clear_rows(t, _):
        for a in range(2):
            for p in range(first, last + 1):
                phi[t, a, p, pl.ds(0, PAD)] = jnp.zeros((PAD, nz), jnp.float32)
                phi[t, a, p, pl.ds(PAD + rows, PAD)] = jnp.zeros((PAD, nz), jnp.float32)
        return 0

    lax.fori_loop(0, STEPS, clear_rows, 0)

    def clear_halo(q):
        def body(t, _):
            for a in range(2):
                phi[t, a, q, pl.ds(PAD, rows)] = jnp.zeros((rows, nz), jnp.float32)
            return 0

        lax.fori_loop(0, STEPS, body, 0)

    @when(jnp.logical_not(has_l))
    def _():
        clear_halo(0)

    @when(jnp.logical_not(has_r))
    def _():
        clear_halo(planes + 1)

    for a, known in ((0, has_dn), (1, has_up)):

        @when(jnp.logical_not(known))
        def _():
            def body(p, _):
                zbuf[a, p] = jnp.zeros((half, nz), jnp.float32)
                return 0

            lax.fori_loop(0, planes, body, 0)

    count = lambda flag: jnp.where(flag, 1, 0)
    expect = 1 + count(has_dn) + count(has_up)
    expect = expect + count(has_l) * (2 - count(in_l)) + count(has_r) * (2 - count(in_r))
    pl.semaphore_wait(barrier, expect)

    for side, known, inside in ((0, has_r, in_r), (1, has_l, in_l)):

        @when(known, jnp.logical_not(inside))
        def _():
            for tgt in range(2):
                halo0(side, tgt).start()

    for i in range(len(parts)):
        for p in range(planes):
            fcopy(i, p, hi).start()
    ccopy(hi).start()

    for copy in loads:
        copy.wait()

    def send_in(a):
        for side, known, inside in ((0, has_r, in_r), (1, has_l, in_l)):

            @when(known, inside)
            def _():
                halo_in(side, a).start()

    send_in(hi)

    def scale(p, _):
        mob[p] = DT * mob[p]
        return 0

    lax.fori_loop(0, planes, scale, 0)

    def begin(k, _):
        a = lax.rem(hi + k, 2)

        @when(k == 1)
        def _():
            for i in range(len(parts)):
                for p in range(planes):
                    fcopy(i, p, other).wait_recv()
            send_in(other)

        for c in range(len(chunks)):
            for p in inner:
                advance(0, a, p, c)

        @when(has_l)
        def _():
            halo_in(0, a).wait_recv()

        @when(has_r)
        def _():
            halo_in(1, a).wait_recv()

        for c in range(len(chunks)):
            advance(0, a, first, c)
            advance(0, a, last, c)
            send_halo(1, a, c)
        return 0

    lax.fori_loop(0, 2, begin, 0)

    def step(t, _):
        def within(k, _):
            a = lax.rem(hi + k, 2)
            for c in range(len(chunks)):
                for p in inner:
                    advance(t, a, p, c)
            return 0

        lax.fori_loop(0, 2, within, 0)

        def rim(k, _):
            a = lax.rem(hi + k, 2)
            for c in range(len(chunks)):
                wait_halo(t, a, c)
                advance(t, a, first, c)
                advance(t, a, last, c)
                send_halo(t + 1, a, c)
            return 0

        lax.fori_loop(0, 2, rim, 0)
        return 0

    lax.fori_loop(1, STEPS - 1, step, 0)

    end = STEPS - 1

    def known_z(a):
        return jnp.logical_and(img - 2 + 4 * a >= 0, img - 2 + 4 * a < images)

    def final_within(k, _):
        a = lax.rem(hi + k, 2)
        for c in range(len(chunks)):
            for p in inner:
                advance(end, a, p, c)

        @when(known_z(a))
        def _():
            for p in inner:
                for c in range(2):
                    zcopy(a, p - 1, c).start()

        return 0

    lax.fori_loop(0, 2, final_within, 0)

    def final_rim(k, _):
        a = lax.rem(hi + k, 2)
        for c in range(len(chunks)):
            wait_halo(end, a, c)
            advance(end, a, first, c)
            advance(end, a, last, c)

        @when(known_z(a))
        def _():
            for p in (first, last):
                for c in range(2):
                    zcopy(a, p - 1, c).start()

        return 0

    lax.fori_loop(0, 2, final_rim, 0)
    ccopy(other).wait_recv()

    def mix(a, p, c):
        at = pl.ds(pl.multiple_of(PAD + h * EXT + c * unit, 8), unit)
        mine = phi[STEPS, a, p + 1, at]
        beside = phi[STEPS, 1 - a, p + 1, at]
        along = zbuf[a, p, pl.ds(pl.multiple_of(c * unit, 8), unit)]
        f = coef[a, 0, pl.ds(0, 1)]
        side = coef[a, 1, pl.ds(0, 1)]
        use_z = jnp.broadcast_to(side, (unit, nz)) == a.astype(jnp.float32)
        return mine + f * (jnp.where(use_z, along, beside) - mine)

    def blend(u, _):
        v = lax.rem(u, 4)
        c = lax.rem(v, 2)
        p = jnp.where(u < 4, 1 + v // 2, 3 * (v // 2))
        for a, known in ((0, has_dn), (1, has_up)):

            @when(known)
            def _():
                zcopy(1 - a, p, c).wait_recv()

        xbuf[p, pl.ds(pl.multiple_of(c * unit, 8), unit)] = mix(other, p, c)
        out[0, p, pl.ds(pl.multiple_of(h * half + c * unit, 8), unit)] = mix(hi, p, c)
        xcopy(p, c, h).start()
        return 0

    lax.fori_loop(0, planes * 2, blend, 0)

    for side, known in ((0, has_r), (1, has_l)):

        @when(known)
        def _():
            for a in range(2):
                halo_in(side, a).wait_send()

            def body(i, _):
                for a in range(2):
                    for c in range(len(chunks)):
                        halo(i, side, a, c).wait_send()
                return 0

            lax.fori_loop(1, STEPS, body, 0)

    for i in range(len(parts)):
        for p in range(planes):
            fcopy(i, p, hi).wait_send()
    ccopy(hi).wait_send()

    def drain(u, _):
        p, c = u // 2, lax.rem(u, 2)
        for a, known in ((0, has_dn), (1, has_up)):

            @when(known)
            def _():
                zcopy(a, p, c).wait_send()

        xcopy(p, c, h).wait_send()
        xcopy(p, c, 1 - h).wait_recv()
        return 0

    lax.fori_loop(0, planes * 2, drain, 0)


def local(images, spaces, field, mobility, fractions, sides):
    _, planes, ny, nz = field.shape
    half = ny // 2
    dma = pltpu.SemaphoreType.DMA
    return pl.pallas_call(
        functools.partial(kernel, (images, spaces, planes, ny, nz)),
        out_shape=jax.ShapeDtypeStruct(field.shape, jnp.float32),
        in_specs=[
            pl.BlockSpec(memory_space=pltpu.HBM),
            pl.BlockSpec(memory_space=pltpu.HBM),
            pl.BlockSpec(memory_space=pltpu.SMEM),
            pl.BlockSpec(memory_space=pltpu.SMEM),
        ],
        out_specs=pl.BlockSpec(memory_space=pltpu.VMEM),
        scratch_shapes=[
            pltpu.VMEM((STEPS + 1, 2, planes + 2, half + EXT + 2 * PAD, nz), jnp.float32),
            pltpu.VMEM((planes, half + EXT, nz), jnp.float32),
            pltpu.VMEM((2, planes, half, nz), jnp.float32),
            pltpu.VMEM((planes, half, nz), jnp.float32),
            pltpu.VMEM((2, 2, 8, nz), jnp.float32),
            dma((planes + 1,)),
            dma,
            dma,
            dma((2, 2)),
            dma((2, 2)),
            dma((STEPS - 1, 2, 2, 2)),
            dma((STEPS - 1, 2, 2, 2)),
            dma((2, planes)),
            dma((2, planes)),
            dma((2, planes, 2)),
            dma((2, planes, 2)),
            dma((planes, 2)),
            dma((planes, 2)),
        ],
        compiler_params=pltpu.CompilerParams(
            collective_id=0, has_side_effects=True, vmem_limit_bytes=50 * 1024 * 1024
        ),
    )(field, mobility, fractions, sides)


def solution(mesh):
    return jax.shard_map(
        functools.partial(local, mesh.shape["image"], mesh.shape["space"]),
        mesh=mesh,
        in_specs=(P("image", "space", None, None), P("space", None, None), P("image"), P("image")),
        out_specs=P("image", "space", None, None),
        check_vma=False,
    )
```

```python
import functools

import jax
import jax.numpy as jnp
from jax import lax
from jax.experimental import pallas as pl
from jax.experimental.pallas import tpu as pltpu
from jax.sharding import PartitionSpec as P

STEPS = 4
DT = 0.1
EPS2 = 1.5
PAD = 8
EXT = 8
CHUNKS = 4
RUN = 4


def kernel(
    cfg, field, mobility, frac, sides, out,
    phi, mob, zbuf, xbuf, coef,
    ls, cs, cr, h0s, h0r, hs, hr, fs, fr, zs, zr, xs, xr,
):
    images, spaces, planes, ny, nz = cfg
    half = ny // 2
    rows = half + EXT
    unit = half // CHUNKS
    first, last = 1, planes
    inner = tuple(range(first + 1, last))
    img = lax.axis_index("image")
    sp = lax.axis_index("space")
    hi = lax.rem(img, 2)
    other = 1 - hi
    z = img // 2
    partner = img + 1 - 2 * hi
    core = lax.rem(sp, 2)
    place = lax.rem(sp, RUN)

    def bound(c, t):
        if c == 0:
            return 0
        if c == CHUNKS:
            return rows
        return c * unit + 8 * STEPS - 8 * t

    def span(c, t):
        return bound(c, t), bound(c + 1, t) - bound(c, t)

    def part(c):
        lo = 0 if c == 0 else min(bound(c, 0) + 8, rows)
        return lo, min(bound(c + 1, 0) + 8, rows) - lo

    def half_of(which, where):
        return lax.rem(which + lax.rem(where // RUN, 2), 2)

    def base_of(h):
        return pl.multiple_of(h * (half - EXT), 8)

    h = half_of(hi, sp)
    has_l = sp > 0
    has_r = sp < spaces - 1
    in_l = core == 1
    in_r = core == 0
    img_l = 2 * z + jnp.where(place == 0, other, hi)
    img_r = 2 * z + jnp.where(place == RUN - 1, other, hi)
    has_dn = z > 0
    has_up = img < images - 2
    mesh_id = pl.DeviceIdType.MESH

    def cells(t, a, p, r, n):
        return phi.at[t, a, p, pl.ds(PAD + r, n)]

    def edge(side):
        return (last, 0, sp + 1) if side == 0 else (first, planes + 1, sp - 1)

    def halo0(side, tgt, c):
        p, q, where = edge(side)
        r, n = span(c, 0)
        return pltpu.make_async_remote_copy(
            src_ref=field.at[0, p - 1, pl.ds(base_of(half_of(tgt, where)) + r, n)],
            dst_ref=cells(0, hi, q, r, n),
            send_sem=h0s.at[side, tgt, c],
            recv_sem=h0r.at[side, hi, c],
            device_id={"image": 2 * z + tgt, "space": where},
            device_id_type=mesh_id,
        )

    def halo_in(side, a, c):
        p, q, where = edge(side)
        r, n = span(c, 0)
        return pltpu.make_async_remote_copy(
            src_ref=cells(0, a, p, r, n),
            dst_ref=cells(0, a, q, r, n),
            send_sem=h0s.at[side, a, c],
            recv_sem=h0r.at[side, a, c],
            device_id={"image": img, "space": where},
            device_id_type=mesh_id,
        )

    def halo(t, side, a, c):
        if t == 0:
            return halo_in(side, a, c)
        p, q, where = edge(side)
        r, n = span(c, t)
        return pltpu.make_async_remote_copy(
            src_ref=cells(t, a, p, r, n),
            dst_ref=cells(t, a, q, r, n),
            send_sem=hs.at[t - 1, side, a, c],
            recv_sem=hr.at[t - 1, side, a, c],
            device_id={"image": img_r if side == 0 else img_l, "space": where},
            device_id_type=mesh_id,
        )

    def fcopy(c, p, a):
        r, n = part(c)
        return pltpu.make_async_remote_copy(
            src_ref=field.at[0, p, pl.ds(base_of(1 - h) + r, n)],
            dst_ref=cells(0, a, p + 1, r, n),
            send_sem=fs.at[c, p],
            recv_sem=fr.at[c, p],
            device_id={"image": partner},
            device_id_type=mesh_id,
        )

    def zcopy(a, p, c):
        return pltpu.make_async_remote_copy(
            src_ref=cells(STEPS, a, p + 1, pl.multiple_of(h * EXT + c * unit, 8), unit),
            dst_ref=zbuf.at[1 - a, p, pl.ds(c * unit, unit)],
            send_sem=zs.at[a, p, c],
            recv_sem=zr.at[1 - a, p, c],
            device_id={"image": img - 2 + 4 * a},
            device_id_type=mesh_id,
        )

    def xcopy(p, c, which):
        return pltpu.make_async_remote_copy(
            src_ref=xbuf.at[p, pl.ds(c * unit, unit)],
            dst_ref=out.at[0, p, pl.ds(pl.multiple_of(which * half + c * unit, 8), unit)],
            send_sem=xs.at[p, c],
            recv_sem=xr.at[p, c],
            device_id={"image": partner},
            device_id_type=mesh_id,
        )

    def ccopy(a):
        return pltpu.make_async_remote_copy(
            src_ref=coef.at[a],
            dst_ref=coef.at[a],
            send_sem=cs,
            recv_sem=cr,
            device_id={"image": partner},
            device_id_type=mesh_id,
        )

    def when(flag, *more):
        for item in more:
            flag = jnp.logical_and(flag, item)
        return pl.when(flag)

    def twice(body):
        def one(k, _):
            body(k, lax.rem(hi + k, 2))
            return 0

        lax.fori_loop(0, 2, one, 0)

    def send_halo(t, a, c):
        @when(has_r)
        def _():
            halo(t, 0, a, c).start()

        @when(has_l)
        def _():
            halo(t, 1, a, c).start()

    def wait_halo(t, a, c):
        @when(has_l)
        def _():
            halo(t, 0, a, c).wait_recv()

        @when(has_r)
        def _():
            halo(t, 1, a, c).wait_recv()

    def send_in(a, c):
        for side, known, inside in ((0, has_r, in_r), (1, has_l, in_l)):

            @when(known, inside)
            def _():
                halo_in(side, a, c).start()

    def advance(t, a, p, r, n):
        lane = lax.broadcasted_iota(jnp.int32, (n, nz), 1)
        here = phi[t, a, p, pl.ds(PAD + r, n)]
        s = phi[t, a, p - 1, pl.ds(PAD + r, n)] + phi[t, a, p + 1, pl.ds(PAD + r, n)]
        wide = phi[t, a, p, pl.ds(PAD + r - 8, n + 16)]
        s = s + wide[7 : 7 + n] + wide[9 : 9 + n]
        s = s + jnp.where(lane == 0, 0.0, pltpu.roll(here, 1, 1))
        s = s + jnp.where(lane == nz - 1, 0.0, pltpu.roll(here, nz - 1, 1))
        m = mob[p - 1, pl.ds(r, n)]
        phi[t + 1, a, p, pl.ds(PAD + r, n)] = here + m * (EPS2 * s - here * (8.0 + here * here))

    loads = [
        pltpu.make_async_copy(field.at[0, p, pl.ds(base_of(h), rows)], cells(0, hi, p + 1, 0, rows), ls.at[p])
        for p in range(planes)
    ]
    loads.append(pltpu.make_async_copy(mobility.at[pl.ds(0, planes), pl.ds(base_of(h), rows)], mob, ls.at[planes]))
    for copy in loads:
        copy.start()

    barrier = pltpu.get_barrier_semaphore()

    def greet(where_img, where_sp):
        pl.semaphore_signal(barrier, 1, device_id={"image": where_img, "space": where_sp}, device_id_type=mesh_id)

    for side, known, inside in ((1, has_l, in_l), (0, has_r, in_r)):
        where = edge(side)[2]

        @when(known, inside)
        def _():
            greet(img, where)

        @when(known, jnp.logical_not(inside))
        def _():
            greet(2 * z, where)
            greet(2 * z + 1, where)

    greet(partner, sp)

    @when(has_dn)
    def _():
        greet(img - 2, sp)

    @when(has_up)
    def _():
        greet(img + 2, sp)

    coef[hi, 0] = jnp.full((8, nz), frac[0], jnp.float32)
    coef[hi, 1] = jnp.full((8, nz), sides[0].astype(jnp.float32), jnp.float32)

    def clear_rows(t, _):
        for a in range(2):
            for p in range(first, last + 1):
                phi[t, a, p, pl.ds(0, PAD)] = jnp.zeros((PAD, nz), jnp.float32)
                phi[t, a, p, pl.ds(PAD + rows, PAD)] = jnp.zeros((PAD, nz), jnp.float32)
        return 0

    lax.fori_loop(0, STEPS, clear_rows, 0)

    def clear_halo(q):
        def body(t, _):
            for a in range(2):
                phi[t, a, q, pl.ds(PAD, rows)] = jnp.zeros((rows, nz), jnp.float32)
            return 0

        lax.fori_loop(0, STEPS, body, 0)

    @when(jnp.logical_not(has_l))
    def _():
        clear_halo(0)

    @when(jnp.logical_not(has_r))
    def _():
        clear_halo(planes + 1)

    for a, known in ((0, has_dn), (1, has_up)):

        @when(jnp.logical_not(known))
        def _():
            def body(p, _):
                zbuf[a, p] = jnp.zeros((half, nz), jnp.float32)
                return 0

            lax.fori_loop(0, planes, body, 0)

    count = lambda flag: jnp.where(flag, 1, 0)
    expect = 1 + count(has_dn) + count(has_up)
    expect = expect + count(has_l) * (2 - count(in_l)) + count(has_r) * (2 - count(in_r))
    pl.semaphore_wait(barrier, expect)

    def issue(c):
        for side, known, inside in ((0, has_r, in_r), (1, has_l, in_l)):

            @when(known, jnp.logical_not(inside))
            def _():
                for tgt in range(2):
                    halo0(side, tgt, c).start()

        if part(c)[1] > 0:
            for p in range(planes):
                fcopy(c, p, hi).start()

    issue(0)
    ccopy(hi).start()
    issue(1)
    for copy in loads:
        copy.wait()
    for c in range(CHUNKS):
        send_in(hi, c)

    def scale(p, _):
        mob[p] = DT * mob[p]
        return 0

    lax.fori_loop(0, planes, scale, 0)

    end = STEPS - 1

    def task(c, t):
        r, n = span(c, t)

        def within(k, a):
            if t == 0:

                @when(k == 1)
                def _():
                    if part(c)[1] > 0:
                        for p in range(planes):
                            fcopy(c, p, other).wait_recv()
                    send_in(other, c)

            for p in inner:
                advance(t, a, p, r, n)

        def rim(k, a):
            wait_halo(t, a, c)
            advance(t, a, first, r, n)
            advance(t, a, last, r, n)
            if t < end:
                send_halo(t + 1, a, c)

        if t == 0:

            def both(k, a):
                within(k, a)
                rim(k, a)

            twice(both)
        else:
            twice(within)
            twice(rim)

    def send_z(c):
        for a, known in ((0, has_dn), (1, has_up)):

            @when(known)
            def _():
                for p in (*(q - 1 for q in inner), first - 1, last - 1):
                    zcopy(a, p, c).start()

    def mix(a, p, c):
        mine = phi[STEPS, a, p + 1, pl.ds(pl.multiple_of(PAD + h * EXT + c * unit, 8), unit)]
        beside = phi[STEPS, 1 - a, p + 1, pl.ds(pl.multiple_of(PAD + h * EXT + c * unit, 8), unit)]
        along = zbuf[a, p, pl.ds(c * unit, unit)]
        f = coef[a, 0, pl.ds(0, 1)]
        side = coef[a, 1, pl.ds(0, 1)]
        use_z = jnp.broadcast_to(side, (unit, nz)) == a.astype(jnp.float32)
        return mine + f * (jnp.where(use_z, along, beside) - mine)

    def blend(c):
        if c == 0:
            ccopy(other).wait_recv()

        def body(i, _):
            p = jnp.where(i < planes - 2, i + 1, (planes - 1) * (i - planes + 2))
            for a, known in ((0, has_dn), (1, has_up)):

                @when(known)
                def _():
                    zcopy(1 - a, p, c).wait_recv()

            xbuf[p, pl.ds(c * unit, unit)] = mix(other, p, c)
            out[0, p, pl.ds(pl.multiple_of(h * half + c * unit, 8), unit)] = mix(hi, p, c)
            xcopy(p, c, h).start()
            return 0

        lax.fori_loop(0, planes, body, 0)

    for wave in range(CHUNKS + STEPS - 1):
        for c in range(CHUNKS):
            t = wave - c
            if 0 <= t < STEPS:
                task(c, t)
                if t == 0 and c + 2 < CHUNKS:
                    issue(c + 2)
                if t == end:
                    send_z(c)
        if wave >= STEPS:
            blend(wave - STEPS)
    blend(CHUNKS - 1)

    for side, known in ((0, has_r), (1, has_l)):

        @when(known)
        def _():
            for t in range(STEPS):
                for c in range(CHUNKS):
                    for a in range(2):
                        halo(t, side, a, c).wait_send()

    for c in range(CHUNKS):
        if part(c)[1] > 0:
            for p in range(planes):
                fcopy(c, p, hi).wait_send()
    ccopy(hi).wait_send()

    def drain(p, _):
        for c in range(CHUNKS):
            for a, known in ((0, has_dn), (1, has_up)):

                @when(known)
                def _():
                    zcopy(a, p, c).wait_send()

            xcopy(p, c, h).wait_send()
            xcopy(p, c, 1 - h).wait_recv()
        return 0

    lax.fori_loop(0, planes, drain, 0)


def local(images, spaces, field, mobility, fractions, sides):
    _, planes, ny, nz = field.shape
    half = ny // 2
    dma = pltpu.SemaphoreType.DMA
    return pl.pallas_call(
        functools.partial(kernel, (images, spaces, planes, ny, nz)),
        out_shape=jax.ShapeDtypeStruct(field.shape, jnp.float32),
        in_specs=[
            pl.BlockSpec(memory_space=pltpu.HBM),
            pl.BlockSpec(memory_space=pltpu.HBM),
            pl.BlockSpec(memory_space=pltpu.SMEM),
            pl.BlockSpec(memory_space=pltpu.SMEM),
        ],
        out_specs=pl.BlockSpec(memory_space=pltpu.VMEM),
        scratch_shapes=[
            pltpu.VMEM((STEPS + 1, 2, planes + 2, half + EXT + 2 * PAD, nz), jnp.float32),
            pltpu.VMEM((planes, half + EXT, nz), jnp.float32),
            pltpu.VMEM((2, planes, half, nz), jnp.float32),
            pltpu.VMEM((planes, half, nz), jnp.float32),
            pltpu.VMEM((2, 2, 8, nz), jnp.float32),
            dma((planes + 1,)),
            dma,
            dma,
            dma((2, 2, CHUNKS)),
            dma((2, 2, CHUNKS)),
            dma((STEPS - 1, 2, 2, CHUNKS)),
            dma((STEPS - 1, 2, 2, CHUNKS)),
            dma((CHUNKS, planes)),
            dma((CHUNKS, planes)),
            dma((2, planes, CHUNKS)),
            dma((2, planes, CHUNKS)),
            dma((planes, CHUNKS)),
            dma((planes, CHUNKS)),
        ],
        compiler_params=pltpu.CompilerParams(
            collective_id=0, has_side_effects=True, vmem_limit_bytes=50 * 1024 * 1024
        ),
    )(field, mobility, fractions, sides)


def solution(mesh):
    return jax.shard_map(
        functools.partial(local, mesh.shape["image"], mesh.shape["space"]),
        mesh=mesh,
        in_specs=(P("image", "space", None, None), P("space", None, None), P("image"), P("image")),
        out_specs=P("image", "space", None, None),
        check_vma=False,
    )
```

```python
import functools

import jax
import jax.numpy as jnp
from jax import lax
from jax.experimental import pallas as pl
from jax.experimental.pallas import tpu as pltpu
from jax.sharding import PartitionSpec as P

STEPS = 4
DT = 0.1
EPS2 = 1.5
PAD = 8
EXT = 8
RUN = 4


def kernel(
    cfg, field, mobility, frac, sides, out,
    phi, mob, zbuf, xbuf, coef,
    ls, cs, cr, h0s, h0r, hs, hr, ns, nr, fs, fr, zs, zr, xs, xr,
):
    images, spaces, planes, ny, nz = cfg
    half = ny // 2
    rows = half + EXT
    unit = half // 2
    chunks = ((0, unit), (unit, rows - unit))
    img = lax.axis_index("image")
    sp = lax.axis_index("space")
    hi = lax.rem(img, 2)
    other = 1 - hi
    z = img // 2
    partner = img + 1 - 2 * hi
    core = lax.rem(sp, 2)
    place = lax.rem(sp, RUN)
    mesh_id = pl.DeviceIdType.MESH

    def half_of(which, where):
        return lax.rem(which + lax.rem(where // RUN, 2), 2)

    def base_of(h):
        return pl.multiple_of(h * (half - EXT), 8)

    h = half_of(hi, sp)
    has_dn = z > 0
    has_up = img < images - 2

    sp_e = sp - 1 + 2 * core
    sp_n = sp + 1 - 2 * core
    has_e = jnp.logical_and(sp_e >= 0, sp_e < spaces)
    crosses = place == core * (RUN - 1)
    img_e = 2 * z + jnp.where(crosses, other, hi)
    slot_e = core * (planes + 1)
    slot_n = (1 - core) * (planes + 1)

    def at(d):
        return core * planes + (1 - 2 * core) * (d + 1) + core

    def cells(t, a, p, r, n):
        return phi.at[t, a, p, pl.ds(PAD + r, n)]

    def halo0(tgt):
        return pltpu.make_async_remote_copy(
            src_ref=field.at[0, at(0) - 1, pl.ds(base_of(half_of(tgt, sp_e)), rows)],
            dst_ref=cells(0, hi, slot_n, 0, rows),
            send_sem=h0s.at[tgt],
            recv_sem=h0r.at[hi],
            device_id={"image": 2 * z + tgt, "space": sp_e},
            device_id_type=mesh_id,
        )

    def halo0_in(a):
        return pltpu.make_async_remote_copy(
            src_ref=cells(0, a, at(0), 0, rows),
            dst_ref=cells(0, a, slot_e, 0, rows),
            send_sem=h0s.at[a],
            recv_sem=h0r.at[a],
            device_id={"image": img_e, "space": sp_e},
            device_id_type=mesh_id,
        )

    def halo(t, a, c, arriving=False):
        r, n = chunks[c]
        return pltpu.make_async_remote_copy(
            src_ref=cells(t, a, at(0), r, n),
            dst_ref=cells(t, a, slot_e if arriving else slot_n, r, n),
            send_sem=hs.at[t - 1, a, c],
            recv_sem=hr.at[t - 1, a, c],
            device_id={"image": img_e, "space": sp_e},
            device_id_type=mesh_id,
        )

    def near(t, a, arriving=False):
        return pltpu.make_async_remote_copy(
            src_ref=cells(t, a, at(planes - 1), 0, rows),
            dst_ref=cells(t, a, slot_n if arriving else slot_e, 0, rows),
            send_sem=ns.at[t, a],
            recv_sem=nr.at[t, a],
            device_id={"space": sp_n},
            device_id_type=mesh_id,
        )

    def fcopy(d, a):
        return pltpu.make_async_remote_copy(
            src_ref=field.at[0, at(d) - 1, pl.ds(base_of(1 - h), rows)],
            dst_ref=cells(0, a, at(d), 0, rows),
            send_sem=fs.at[d],
            recv_sem=fr.at[d],
            device_id={"image": partner},
            device_id_type=mesh_id,
        )

    def zcopy(a, d, c):
        return pltpu.make_async_remote_copy(
            src_ref=cells(STEPS, a, at(d), pl.multiple_of(h * EXT + c * unit, 8), unit),
            dst_ref=zbuf.at[1 - a, d, pl.ds(c * unit, unit)],
            send_sem=zs.at[a, d, c],
            recv_sem=zr.at[1 - a, d, c],
            device_id={"image": img - 2 + 4 * a},
            device_id_type=mesh_id,
        )

    def xcopy(d, c, which):
        return pltpu.make_async_remote_copy(
            src_ref=xbuf.at[d, pl.ds(c * unit, unit)],
            dst_ref=out.at[0, at(d) - 1, pl.ds(pl.multiple_of(which * half + c * unit, 8), unit)],
            send_sem=xs.at[d, c],
            recv_sem=xr.at[d, c],
            device_id={"image": partner},
            device_id_type=mesh_id,
        )

    def ccopy(a):
        return pltpu.make_async_remote_copy(
            src_ref=coef.at[a],
            dst_ref=coef.at[a],
            send_sem=cs,
            recv_sem=cr,
            device_id={"image": partner},
            device_id_type=mesh_id,
        )

    def when(flag, *more):
        for item in more:
            flag = jnp.logical_and(flag, item)
        return pl.when(flag)

    def loop(lo, hi_, body):
        def one(i, _):
            body(i)
            return 0

        lax.fori_loop(lo, hi_, one, 0)

    def twice(body):
        loop(0, 2, lambda k: body(k, lax.rem(hi + k, 2)))

    def advance(t, a, d, r, n):
        p = at(d)
        lane = lax.broadcasted_iota(jnp.int32, (n, nz), 1)
        here = phi[t, a, p, pl.ds(PAD + r, n)]
        s = phi[t, a, p - 1, pl.ds(PAD + r, n)] + phi[t, a, p + 1, pl.ds(PAD + r, n)]
        wide = phi[t, a, p, pl.ds(PAD + r - 8, n + 16)]
        s = s + wide[7 : 7 + n] + wide[9 : 9 + n]
        s = s + jnp.where(lane == 0, 0.0, pltpu.roll(here, 1, 1))
        s = s + jnp.where(lane == nz - 1, 0.0, pltpu.roll(here, nz - 1, 1))
        m = mob[p - 1, pl.ds(r, n)]
        phi[t + 1, a, p, pl.ds(PAD + r, n)] = here + m * (EPS2 * s - here * (8.0 + here * here))

    def whole(t, a, d):
        advance(t, a, d, 0, rows)

    loads = [
        pltpu.make_async_copy(field.at[0, p, pl.ds(base_of(h), rows)], cells(0, hi, p + 1, 0, rows), ls.at[p])
        for p in range(planes)
    ]
    loads.append(pltpu.make_async_copy(mobility.at[pl.ds(0, planes), pl.ds(base_of(h), rows)], mob, ls.at[planes]))
    for copy in loads:
        copy.start()

    barrier = pltpu.get_barrier_semaphore()

    def greet(where_img, where_sp):
        pl.semaphore_signal(barrier, 1, device_id={"image": where_img, "space": where_sp}, device_id_type=mesh_id)

    @when(has_e)
    def _():
        greet(2 * z, sp_e)
        greet(2 * z + 1, sp_e)

    greet(partner, sp)
    greet(img, sp_n)

    @when(has_dn)
    def _():
        greet(img - 2, sp)

    @when(has_up)
    def _():
        greet(img + 2, sp)

    coef[hi, 0] = jnp.full((8, nz), frac[0], jnp.float32)
    coef[hi, 1] = jnp.full((8, nz), sides[0].astype(jnp.float32), jnp.float32)

    def clear_rows(t):
        for a in range(2):
            for p in range(1, planes + 1):
                phi[t, a, p, pl.ds(0, PAD)] = jnp.zeros((PAD, nz), jnp.float32)
                phi[t, a, p, pl.ds(PAD + rows, PAD)] = jnp.zeros((PAD, nz), jnp.float32)

    loop(0, STEPS, clear_rows)

    @when(jnp.logical_not(has_e))
    def _():
        def body(t):
            for a in range(2):
                phi[t, a, slot_e, pl.ds(PAD, rows)] = jnp.zeros((rows, nz), jnp.float32)

        loop(0, STEPS, body)

    for a, known in ((0, has_dn), (1, has_up)):

        @when(jnp.logical_not(known))
        def _():
            def body(d):
                zbuf[a, d] = jnp.zeros((half, nz), jnp.float32)

            loop(0, planes, body)

    count = lambda flag: jnp.where(flag, 1, 0)
    pl.semaphore_wait(barrier, 2 + count(has_dn) + count(has_up) + 2 * count(has_e))

    @when(has_e)
    def _():
        for tgt in range(2):
            halo0(tgt).start()

    early = planes // 2
    for d in range(early):
        fcopy(d, hi).start()
    ccopy(hi).start()
    for copy in loads:
        copy.wait()
    near(0, hi).start()

    def scale(p):
        mob[p] = DT * mob[p]

    loop(0, planes, scale)

    def send_z(a, d):
        @when(img - 2 + 4 * a >= 0, img - 2 + 4 * a < images)
        def _():
            for c in range(2):
                zcopy(a, d, c).start()

    def begin(k, a):
        @when(k == 1)
        def _():
            for d in range(early):
                fcopy(d, other).wait_recv()

        @when(has_e)
        def _():
            halo0_in(a).wait_recv()

        for c in range(len(chunks)):
            advance(0, a, 0, *chunks[c])

            @when(has_e)
            def _():
                halo(1, a, c).start()

        @when(k == 0)
        def _():
            for d in range(early, planes):
                fcopy(d, hi).start()

        @when(k == 1)
        def _():
            for d in range(early, planes):
                fcopy(d, other).wait_recv()
            near(0, other).start()

        def deeper(t):
            near(t, a, True).wait_recv()
            whole(t, a, planes - 1)

            @when(t < STEPS - 1)
            def _():
                near(t + 1, a).start()

            loop(0, planes - 1 - jnp.maximum(t, 1), lambda i: whole(t, a, planes - 2 - i))

        loop(0, STEPS, deeper)
        send_z(a, planes - 1)

    twice(begin)

    def mix(a, d, c):
        p = at(d)
        here = pl.ds(pl.multiple_of(PAD + h * EXT + c * unit, 8), unit)
        mine = phi[STEPS, a, p, here]
        beside = phi[STEPS, 1 - a, p, here]
        along = zbuf[a, d, pl.ds(c * unit, unit)]
        f = coef[a, 0, pl.ds(0, 1)]
        side = coef[a, 1, pl.ds(0, 1)]
        use_z = jnp.broadcast_to(side, (unit, nz)) == a.astype(jnp.float32)
        return mine + f * (jnp.where(use_z, along, beside) - mine)

    def blend(d):
        for c in range(2):
            for a, known in ((0, has_dn), (1, has_up)):

                @when(known)
                def _():
                    zcopy(1 - a, d, c).wait_recv()

            xbuf[d, pl.ds(c * unit, unit)] = mix(other, d, c)
            out[0, at(d) - 1, pl.ds(pl.multiple_of(h * half + c * unit, 8), unit)] = mix(hi, d, c)
            xcopy(d, c, h).start()

    ccopy(other).wait_recv()

    def extend(r):
        def face(k, a):
            for c in range(len(chunks)):

                @when(has_e)
                def _():
                    halo(r, a, c, True).wait_recv()

                advance(r, a, 0, *chunks[c])

                @when(has_e, r < STEPS - 1)
                def _():
                    halo(r + 1, a, c).start()

        twice(face)

        def behind(k, a):
            loop(1, STEPS - r, lambda j: whole(r + j, a, j))
            send_z(a, STEPS - 1 - r)

        twice(behind)
        blend(STEPS - r)

    loop(1, STEPS, extend)
    blend(0)

    @when(has_e)
    def _():
        for tgt in range(2):
            halo0(tgt).wait_send()

        def body(t):
            for a in range(2):
                for c in range(len(chunks)):
                    halo(t, a, c).wait_send()

        loop(1, STEPS, body)

    def sent(t):
        for a in range(2):
            near(t, a).wait_send()

    loop(0, STEPS, sent)
    ccopy(hi).wait_send()

    def drain(d):
        fcopy(d, hi).wait_send()
        for c in range(2):
            for a, known in ((0, has_dn), (1, has_up)):

                @when(known)
                def _():
                    zcopy(a, d, c).wait_send()

            xcopy(d, c, h).wait_send()
            xcopy(d, c, 1 - h).wait_recv()

    loop(0, planes, drain)


def local(images, spaces, field, mobility, fractions, sides):
    _, planes, ny, nz = field.shape
    half = ny // 2
    dma = pltpu.SemaphoreType.DMA
    return pl.pallas_call(
        functools.partial(kernel, (images, spaces, planes, ny, nz)),
        out_shape=jax.ShapeDtypeStruct(field.shape, jnp.float32),
        in_specs=[
            pl.BlockSpec(memory_space=pltpu.HBM),
            pl.BlockSpec(memory_space=pltpu.HBM),
            pl.BlockSpec(memory_space=pltpu.SMEM),
            pl.BlockSpec(memory_space=pltpu.SMEM),
        ],
        out_specs=pl.BlockSpec(memory_space=pltpu.VMEM),
        scratch_shapes=[
            pltpu.VMEM((STEPS + 1, 2, planes + 2, half + EXT + 2 * PAD, nz), jnp.float32),
            pltpu.VMEM((planes, half + EXT, nz), jnp.float32),
            pltpu.VMEM((2, planes, half, nz), jnp.float32),
            pltpu.VMEM((planes, half, nz), jnp.float32),
            pltpu.VMEM((2, 2, 8, nz), jnp.float32),
            dma((planes + 1,)),
            dma,
            dma,
            dma((2,)),
            dma((2,)),
            dma((STEPS - 1, 2, 2)),
            dma((STEPS - 1, 2, 2)),
            dma((STEPS, 2)),
            dma((STEPS, 2)),
            dma((planes,)),
            dma((planes,)),
            dma((2, planes, 2)),
            dma((2, planes, 2)),
            dma((planes, 2)),
            dma((planes, 2)),
        ],
        compiler_params=pltpu.CompilerParams(
            collective_id=0, has_side_effects=True, vmem_limit_bytes=50 * 1024 * 1024
        ),
    )(field, mobility, fractions, sides)


def solution(mesh):
    return jax.shard_map(
        functools.partial(local, mesh.shape["image"], mesh.shape["space"]),
        mesh=mesh,
        in_specs=(P("image", "space", None, None), P("space", None, None), P("image"), P("image")),
        out_specs=P("image", "space", None, None),
        check_vma=False,
    )
```

```python
import functools

import jax
import jax.numpy as jnp
from jax import lax
from jax.experimental import pallas as pl
from jax.experimental.pallas import tpu as pltpu
from jax.sharding import PartitionSpec as P

STEPS = 4
DT = 0.1
EPS2 = 1.5
PAD = 8
EXT = 8
RUN = 4


def kernel(
    cfg, field, mobility, frac, sides, out,
    phi, mob, zbuf, xbuf, coef,
    ls, cs, cr, h0s, h0r, hs, hr, fs, fr, zs, zr, xs, xr,
):
    images, spaces, planes, ny, nz = cfg
    half = ny // 2
    rows = half + EXT
    unit = half // 2
    chunks = ((0, unit), (unit, rows - unit))
    parts = ((0, unit + 8), (unit + 8, rows - unit - 8))
    first, last = 1, planes
    img = lax.axis_index("image")
    sp = lax.axis_index("space")
    hi = lax.rem(img, 2)
    other = 1 - hi
    z = img // 2
    partner = img + 1 - 2 * hi
    core = lax.rem(sp, 2)
    place = lax.rem(sp, RUN)

    def half_of(which, where):
        return lax.rem(which + lax.rem(where // RUN, 2), 2)

    def base_of(h):
        return pl.multiple_of(h * (half - EXT), 8)

    h = half_of(hi, sp)
    has_l = sp > 0
    has_r = sp < spaces - 1
    in_l = core == 1
    in_r = core == 0
    img_l = 2 * z + jnp.where(place == 0, other, hi)
    img_r = 2 * z + jnp.where(place == RUN - 1, other, hi)
    has_dn = z > 0
    has_up = img < images - 2
    mesh_id = pl.DeviceIdType.MESH

    def cells(t, a, p, r, n):
        return phi.at[t, a, p, pl.ds(PAD + r, n)]

    def edge(side):
        return (last, 0, sp + 1) if side == 0 else (first, planes + 1, sp - 1)

    def halo0(side, tgt):
        p, q, where = edge(side)
        return pltpu.make_async_remote_copy(
            src_ref=field.at[0, p - 1, pl.ds(base_of(half_of(tgt, where)), rows)],
            dst_ref=cells(0, hi, q, 0, rows),
            send_sem=h0s.at[side, tgt],
            recv_sem=h0r.at[side, hi],
            device_id={"image": 2 * z + tgt, "space": where},
            device_id_type=mesh_id,
        )

    def halo_in(side, a):
        p, q, where = edge(side)
        return pltpu.make_async_remote_copy(
            src_ref=cells(0, a, p, 0, rows),
            dst_ref=cells(0, a, q, 0, rows),
            send_sem=h0s.at[side, a],
            recv_sem=h0r.at[side, a],
            device_id={"image": img, "space": where},
            device_id_type=mesh_id,
        )

    def halo(t, side, a, c):
        p, q, where = edge(side)
        r, n = chunks[c]
        return pltpu.make_async_remote_copy(
            src_ref=cells(t, a, p, r, n),
            dst_ref=cells(t, a, q, r, n),
            send_sem=hs.at[t - 1, side, a, c],
            recv_sem=hr.at[t - 1, side, a, c],
            device_id={"image": img_r if side == 0 else img_l, "space": where},
            device_id_type=mesh_id,
        )

    def fcopy(i, p, a):
        r, n = parts[i]
        return pltpu.make_async_remote_copy(
            src_ref=field.at[0, p, pl.ds(base_of(1 - h) + r, n)],
            dst_ref=cells(0, a, p + 1, r, n),
            send_sem=fs.at[i, p],
            recv_sem=fr.at[i, p],
            device_id={"image": partner},
            device_id_type=mesh_id,
        )

    def rows_of(ref, k, p, c):
        return ref.at[k, p, pl.ds(pl.multiple_of(c * unit, 8), unit)]

    def zcopy(a, p, c):
        return pltpu.make_async_remote_copy(
            src_ref=cells(STEPS, a, p + 1, pl.multiple_of(h * EXT + c * unit, 8), unit),
            dst_ref=rows_of(zbuf, 1 - a, p, c),
            send_sem=zs.at[a, p, c],
            recv_sem=zr.at[1 - a, p, c],
            device_id={"image": img - 2 + 4 * a},
            device_id_type=mesh_id,
        )

    def xcopy(p, c, which):
        return pltpu.make_async_remote_copy(
            src_ref=xbuf.at[p, pl.ds(pl.multiple_of(c * unit, 8), unit)],
            dst_ref=out.at[0, p, pl.ds(pl.multiple_of(which * half + c * unit, 8), unit)],
            send_sem=xs.at[p, c],
            recv_sem=xr.at[p, c],
            device_id={"image": partner},
            device_id_type=mesh_id,
        )

    def ccopy(a):
        return pltpu.make_async_remote_copy(
            src_ref=coef.at[a],
            dst_ref=coef.at[a],
            send_sem=cs,
            recv_sem=cr,
            device_id={"image": partner},
            device_id_type=mesh_id,
        )

    def when(flag, *more):
        for item in more:
            flag = jnp.logical_and(flag, item)
        return pl.when(flag)

    def send_halo(t, a, c):
        @when(has_r)
        def _():
            halo(t, 0, a, c).start()

        @when(has_l)
        def _():
            halo(t, 1, a, c).start()

    def wait_halo(t, a, c):
        @when(has_l)
        def _():
            halo(t, 0, a, c).wait_recv()

        @when(has_r)
        def _():
            halo(t, 1, a, c).wait_recv()

    def advance(t, a, p, c):
        r, n = chunks[c]
        lane = lax.broadcasted_iota(jnp.int32, (n, nz), 1)
        here = phi[t, a, p, pl.ds(PAD + r, n)]
        s = phi[t, a, p - 1, pl.ds(PAD + r, n)] + phi[t, a, p + 1, pl.ds(PAD + r, n)]
        wide = phi[t, a, p, pl.ds(PAD + r - 8, n + 16)]
        s = s + wide[7 : 7 + n] + wide[9 : 9 + n]
        s = s + jnp.where(lane == 0, 0.0, pltpu.roll(here, 1, 1))
        s = s + jnp.where(lane == nz - 1, 0.0, pltpu.roll(here, nz - 1, 1))
        m = mob[p - 1, pl.ds(r, n)]
        phi[t + 1, a, p, pl.ds(PAD + r, n)] = here + m * (EPS2 * s - here * (8.0 + here * here))

    inner = tuple(range(first + 1, last))

    loads = [
        pltpu.make_async_copy(field.at[0, p, pl.ds(base_of(h), rows)], cells(0, hi, p + 1, 0, rows), ls.at[p])
        for p in range(planes)
    ]
    loads.append(pltpu.make_async_copy(mobility.at[pl.ds(0, planes), pl.ds(base_of(h), rows)], mob, ls.at[planes]))
    for copy in loads:
        copy.start()

    barrier = pltpu.get_barrier_semaphore()

    def greet(where_img, where_sp):
        pl.semaphore_signal(barrier, 1, device_id={"image": where_img, "space": where_sp}, device_id_type=mesh_id)

    for side, known, inside in ((1, has_l, in_l), (0, has_r, in_r)):
        where = edge(side)[2]

        @when(known, inside)
        def _():
            greet(img, where)

        @when(known, jnp.logical_not(inside))
        def _():
            greet(2 * z, where)
            greet(2 * z + 1, where)

    greet(partner, sp)

    @when(has_dn)
    def _():
        greet(img - 2, sp)

    @when(has_up)
    def _():
        greet(img + 2, sp)

    coef[hi, 0] = jnp.full((8, nz), frac[0], jnp.float32)
    coef[hi, 1] = jnp.full((8, nz), sides[0].astype(jnp.float32), jnp.float32)

    def clear_rows(t, _):
        for a in range(2):
            for p in range(first, last + 1):
                phi[t, a, p, pl.ds(0, PAD)] = jnp.zeros((PAD, nz), jnp.float32)
                phi[t, a, p, pl.ds(PAD + rows, PAD)] = jnp.zeros((PAD, nz), jnp.float32)
        return 0

    lax.fori_loop(0, STEPS, clear_rows, 0)

    def clear_halo(q):
        def body(t, _):
            for a in range(2):
                phi[t, a, q, pl.ds(PAD, rows)] = jnp.zeros((rows, nz), jnp.float32)
            return 0

        lax.fori_loop(0, STEPS, body, 0)

    @when(jnp.logical_not(has_l))
    def _():
        clear_halo(0)

    @when(jnp.logical_not(has_r))
    def _():
        clear_halo(planes + 1)

    for a, known in ((0, has_dn), (1, has_up)):

        @when(jnp.logical_not(known))
        def _():
            def body(p, _):
                zbuf[a, p] = jnp.zeros((half, nz), jnp.float32)
                return 0

            lax.fori_loop(0, planes, body, 0)

    count = lambda flag: jnp.where(flag, 1, 0)
    expect = 1 + count(has_dn) + count(has_up)
    expect = expect + count(has_l) * (2 - count(in_l)) + count(has_r) * (2 - count(in_r))
    pl.semaphore_wait(barrier, expect)

    for side, known, inside in ((0, has_r, in_r), (1, has_l, in_l)):

        @when(known, jnp.logical_not(inside))
        def _():
            for tgt in range(2):
                halo0(side, tgt).start()

    for i in range(len(parts)):
        for p in range(planes):
            fcopy(i, p, hi).start()
    ccopy(hi).start()

    for copy in loads:
        copy.wait()

    def send_in(a):
        for side, known, inside in ((0, has_r, in_r), (1, has_l, in_l)):

            @when(known, inside)
            def _():
                halo_in(side, a).start()

    send_in(hi)

    def scale(p, _):
        mob[p] = DT * mob[p]
        return 0

    lax.fori_loop(0, planes, scale, 0)

    def begin(k, _):
        a = lax.rem(hi + k, 2)

        @when(k == 1)
        def _():
            for i in range(len(parts)):
                for p in range(planes):
                    fcopy(i, p, other).wait_recv()
            send_in(other)

        for c in range(len(chunks)):
            for p in inner:
                advance(0, a, p, c)

        @when(has_l)
        def _():
            halo_in(0, a).wait_recv()

        @when(has_r)
        def _():
            halo_in(1, a).wait_recv()

        for c in range(len(chunks)):
            advance(0, a, first, c)
            advance(0, a, last, c)
            send_halo(1, a, c)
        return 0

    lax.fori_loop(0, 2, begin, 0)

    def step(t, _):
        def within(k, _):
            a = k
            for c in range(len(chunks)):
                for p in inner:
                    advance(t, a, p, c)
            return 0

        lax.fori_loop(0, 2, within, 0)

        def rim(k, _):
            a = k
            for c in range(len(chunks)):
                wait_halo(t, a, c)
                advance(t, a, first, c)
                advance(t, a, last, c)
                send_halo(t + 1, a, c)
            return 0

        lax.fori_loop(0, 2, rim, 0)
        return 0

    lax.fori_loop(1, STEPS - 1, step, 0)

    end = STEPS - 1

    def known_z(a):
        return jnp.logical_and(img - 2 + 4 * a >= 0, img - 2 + 4 * a < images)

    def final_within(k, _):
        a = k
        for c in range(len(chunks)):
            for p in inner:
                advance(end, a, p, c)

        @when(known_z(a))
        def _():
            for p in inner:
                for c in range(2):
                    zcopy(a, p - 1, c).start()

        return 0

    lax.fori_loop(0, 2, final_within, 0)

    def final_rim(k, _):
        a = k
        for c in range(len(chunks)):
            wait_halo(end, a, c)
            advance(end, a, first, c)
            advance(end, a, last, c)

        @when(known_z(a))
        def _():
            for p in (first, last):
                for c in range(2):
                    zcopy(a, p - 1, c).start()

        return 0

    lax.fori_loop(0, 2, final_rim, 0)
    ccopy(other).wait_recv()

    def mix(a, p, c):
        at = pl.ds(pl.multiple_of(PAD + h * EXT + c * unit, 8), unit)
        mine = phi[STEPS, a, p + 1, at]
        beside = phi[STEPS, 1 - a, p + 1, at]
        along = zbuf[a, p, pl.ds(pl.multiple_of(c * unit, 8), unit)]
        f = coef[a, 0, pl.ds(0, 1)]
        side = coef[a, 1, pl.ds(0, 1)]
        use_z = jnp.broadcast_to(side, (unit, nz)) == a.astype(jnp.float32)
        return mine + f * (jnp.where(use_z, along, beside) - mine)

    def blend(u, _):
        v = lax.rem(u, 4)
        c = lax.rem(v, 2)
        p = jnp.where(u < 4, 1 + v // 2, 3 * (v // 2))
        for a, known in ((0, has_dn), (1, has_up)):

            @when(known)
            def _():
                zcopy(1 - a, p, c).wait_recv()

        xbuf[p, pl.ds(pl.multiple_of(c * unit, 8), unit)] = mix(other, p, c)
        out[0, p, pl.ds(pl.multiple_of(h * half + c * unit, 8), unit)] = mix(hi, p, c)
        xcopy(p, c, h).start()
        return 0

    lax.fori_loop(0, planes * 2, blend, 0)

    for side, known in ((0, has_r), (1, has_l)):

        @when(known)
        def _():
            for a in range(2):
                halo_in(side, a).wait_send()

            def body(i, _):
                for a in range(2):
                    for c in range(len(chunks)):
                        halo(i, side, a, c).wait_send()
                return 0

            lax.fori_loop(1, STEPS, body, 0)

    for i in range(len(parts)):
        for p in range(planes):
            fcopy(i, p, hi).wait_send()
    ccopy(hi).wait_send()

    def drain(u, _):
        p, c = u // 2, lax.rem(u, 2)
        for a, known in ((0, has_dn), (1, has_up)):

            @when(known)
            def _():
                zcopy(a, p, c).wait_send()

        xcopy(p, c, h).wait_send()
        xcopy(p, c, 1 - h).wait_recv()
        return 0

    lax.fori_loop(0, planes * 2, drain, 0)


def local(images, spaces, field, mobility, fractions, sides):
    _, planes, ny, nz = field.shape
    half = ny // 2
    dma = pltpu.SemaphoreType.DMA
    return pl.pallas_call(
        functools.partial(kernel, (images, spaces, planes, ny, nz)),
        out_shape=jax.ShapeDtypeStruct(field.shape, jnp.float32),
        in_specs=[
            pl.BlockSpec(memory_space=pltpu.HBM),
            pl.BlockSpec(memory_space=pltpu.HBM),
            pl.BlockSpec(memory_space=pltpu.SMEM),
            pl.BlockSpec(memory_space=pltpu.SMEM),
        ],
        out_specs=pl.BlockSpec(memory_space=pltpu.VMEM),
        scratch_shapes=[
            pltpu.VMEM((STEPS + 1, 2, planes + 2, half + EXT + 2 * PAD, nz), jnp.float32),
            pltpu.VMEM((planes, half + EXT, nz), jnp.float32),
            pltpu.VMEM((2, planes, half, nz), jnp.float32),
            pltpu.VMEM((planes, half, nz), jnp.float32),
            pltpu.VMEM((2, 2, 8, nz), jnp.float32),
            dma((planes + 1,)),
            dma,
            dma,
            dma((2, 2)),
            dma((2, 2)),
            dma((STEPS - 1, 2, 2, 2)),
            dma((STEPS - 1, 2, 2, 2)),
            dma((2, planes)),
            dma((2, planes)),
            dma((2, planes, 2)),
            dma((2, planes, 2)),
            dma((planes, 2)),
            dma((planes, 2)),
        ],
        compiler_params=pltpu.CompilerParams(
            collective_id=0, has_side_effects=True, vmem_limit_bytes=50 * 1024 * 1024
        ),
    )(field, mobility, fractions, sides)


def solution(mesh):
    return jax.shard_map(
        functools.partial(local, mesh.shape["image"], mesh.shape["space"]),
        mesh=mesh,
        in_specs=(P("image", "space", None, None), P("space", None, None), P("image"), P("image")),
        out_specs=P("image", "space", None, None),
        check_vma=False,
    )
```

```python
import functools

import jax
import jax.numpy as jnp
from jax import lax
from jax.experimental import pallas as pl
from jax.experimental.pallas import tpu as pltpu
from jax.sharding import PartitionSpec as P

STEPS = 4
DT = 0.1
EPS2 = 1.5
PAD = 8
EXT = 8
RUN = 4


def kernel(
    cfg, field, mobility, frac, sides, out,
    phi, mob, zbuf, xbuf, coef,
    ls, cs, cr, h0s, h0r, hs, hr, fs, fr, zs, zr, xs, xr,
):
    images, spaces, planes, ny, nz = cfg
    half = ny // 2
    rows = half + EXT
    unit = half // 2
    chunks = ((0, unit), (unit, rows - unit))
    parts = ((0, unit + 8), (unit + 8, rows - unit - 8))
    first, last = 1, planes
    img = lax.axis_index("image")
    sp = lax.axis_index("space")
    hi = lax.rem(img, 2)
    other = 1 - hi
    z = img // 2
    partner = img + 1 - 2 * hi
    core = lax.rem(sp, 2)
    place = lax.rem(sp, RUN)

    def half_of(which, where):
        return lax.rem(which + lax.rem(where // RUN, 2), 2)

    def base_of(h):
        return pl.multiple_of(h * (half - EXT), 8)

    h = half_of(hi, sp)
    has_l = sp > 0
    has_r = sp < spaces - 1
    in_l = core == 1
    in_r = core == 0
    img_l = 2 * z + jnp.where(place == 0, other, hi)
    img_r = 2 * z + jnp.where(place == RUN - 1, other, hi)
    has_dn = z > 0
    has_up = img < images - 2
    mesh_id = pl.DeviceIdType.MESH

    def cells(t, a, p, r, n):
        return phi.at[t, a, p, pl.ds(PAD + r, n)]

    def edge(side):
        return (last, 0, sp + 1) if side == 0 else (first, planes + 1, sp - 1)

    def halo0(side, tgt):
        p, q, where = edge(side)
        return pltpu.make_async_remote_copy(
            src_ref=field.at[0, p - 1, pl.ds(base_of(half_of(tgt, where)), rows)],
            dst_ref=cells(0, hi, q, 0, rows),
            send_sem=h0s.at[side, tgt],
            recv_sem=h0r.at[side, hi],
            device_id={"image": 2 * z + tgt, "space": where},
            device_id_type=mesh_id,
        )

    def halo_in(side, a):
        p, q, where = edge(side)
        return pltpu.make_async_remote_copy(
            src_ref=cells(0, a, p, 0, rows),
            dst_ref=cells(0, a, q, 0, rows),
            send_sem=h0s.at[side, a],
            recv_sem=h0r.at[side, a],
            device_id={"image": img, "space": where},
            device_id_type=mesh_id,
        )

    def halo(t, side, a, c):
        p, q, where = edge(side)
        r, n = chunks[c]
        return pltpu.make_async_remote_copy(
            src_ref=cells(t, a, p, r, n),
            dst_ref=cells(t, a, q, r, n),
            send_sem=hs.at[t - 1, side, a, c],
            recv_sem=hr.at[t - 1, side, a, c],
            device_id={"image": img_r if side == 0 else img_l, "space": where},
            device_id_type=mesh_id,
        )

    def fcopy(i, p, a):
        r, n = parts[i]
        return pltpu.make_async_remote_copy(
            src_ref=field.at[0, p, pl.ds(base_of(1 - h) + r, n)],
            dst_ref=cells(0, a, p + 1, r, n),
            send_sem=fs.at[i, p],
            recv_sem=fr.at[i, p],
            device_id={"image": partner},
            device_id_type=mesh_id,
        )

    def rows_of(ref, k, p, c):
        return ref.at[k, p, pl.ds(pl.multiple_of(c * unit, 8), unit)]

    def zcopy(a, p, c):
        return pltpu.make_async_remote_copy(
            src_ref=cells(STEPS, a, p + 1, pl.multiple_of(h * EXT + c * unit, 8), unit),
            dst_ref=rows_of(zbuf, 1 - a, p, c),
            send_sem=zs.at[a, p, c],
            recv_sem=zr.at[1 - a, p, c],
            device_id={"image": img - 2 + 4 * a},
            device_id_type=mesh_id,
        )

    def xcopy(p, c, which):
        return pltpu.make_async_remote_copy(
            src_ref=xbuf.at[p, pl.ds(pl.multiple_of(c * unit, 8), unit)],
            dst_ref=out.at[0, p, pl.ds(pl.multiple_of(which * half + c * unit, 8), unit)],
            send_sem=xs.at[p, c],
            recv_sem=xr.at[p, c],
            device_id={"image": partner},
            device_id_type=mesh_id,
        )

    def ccopy(a):
        return pltpu.make_async_remote_copy(
            src_ref=coef.at[a],
            dst_ref=coef.at[a],
            send_sem=cs,
            recv_sem=cr,
            device_id={"image": partner},
            device_id_type=mesh_id,
        )

    def when(flag, *more):
        for item in more:
            flag = jnp.logical_and(flag, item)
        return pl.when(flag)

    def wait_halo(t, a, c):
        @when(has_l)
        def _():
            halo(t, 0, a, c).wait_recv()

        @when(has_r)
        def _():
            halo(t, 1, a, c).wait_recv()

    outer = jnp.where(core == 0, first, last)
    near = first + last - outer

    def send_face(t, a, c, out_side):
        @when(core == (1 if out_side else 0), has_r)
        def _():
            halo(t, 0, a, c).start()

        @when(core == (0 if out_side else 1), has_l)
        def _():
            halo(t, 1, a, c).start()

    def wait_face(copy, out_side):
        @when(core == (0 if out_side else 1), has_l)
        def _():
            copy(0).wait_recv()

        @when(core == (1 if out_side else 0), has_r)
        def _():
            copy(1).wait_recv()

    def advance(t, a, p, c):
        r, n = chunks[c]
        lane = lax.broadcasted_iota(jnp.int32, (n, nz), 1)
        here = phi[t, a, p, pl.ds(PAD + r, n)]
        s = phi[t, a, p - 1, pl.ds(PAD + r, n)] + phi[t, a, p + 1, pl.ds(PAD + r, n)]
        wide = phi[t, a, p, pl.ds(PAD + r - 8, n + 16)]
        s = s + wide[7 : 7 + n] + wide[9 : 9 + n]
        s = s + jnp.where(lane == 0, 0.0, pltpu.roll(here, 1, 1))
        s = s + jnp.where(lane == nz - 1, 0.0, pltpu.roll(here, nz - 1, 1))
        m = mob[p - 1, pl.ds(r, n)]
        phi[t + 1, a, p, pl.ds(PAD + r, n)] = here + m * (EPS2 * s - here * (8.0 + here * here))

    inner = tuple(range(first + 1, last))

    loads = [
        pltpu.make_async_copy(field.at[0, p, pl.ds(base_of(h), rows)], cells(0, hi, p + 1, 0, rows), ls.at[p])
        for p in range(planes)
    ]
    loads.append(pltpu.make_async_copy(mobility.at[pl.ds(0, planes), pl.ds(base_of(h), rows)], mob, ls.at[planes]))
    for copy in loads:
        copy.start()

    barrier = pltpu.get_barrier_semaphore()

    def greet(where_img, where_sp):
        pl.semaphore_signal(barrier, 1, device_id={"image": where_img, "space": where_sp}, device_id_type=mesh_id)

    for side, known, inside in ((1, has_l, in_l), (0, has_r, in_r)):
        where = edge(side)[2]

        @when(known, inside)
        def _():
            greet(img, where)

        @when(known, jnp.logical_not(inside))
        def _():
            greet(2 * z, where)
            greet(2 * z + 1, where)

    greet(partner, sp)

    @when(has_dn)
    def _():
        greet(img - 2, sp)

    @when(has_up)
    def _():
        greet(img + 2, sp)

    coef[hi, 0] = jnp.full((8, nz), frac[0], jnp.float32)
    coef[hi, 1] = jnp.full((8, nz), sides[0].astype(jnp.float32), jnp.float32)

    def clear_rows(t, _):
        for a in range(2):
            for p in range(first, last + 1):
                phi[t, a, p, pl.ds(0, PAD)] = jnp.zeros((PAD, nz), jnp.float32)
                phi[t, a, p, pl.ds(PAD + rows, PAD)] = jnp.zeros((PAD, nz), jnp.float32)
        return 0

    lax.fori_loop(0, STEPS, clear_rows, 0)

    def clear_halo(q):
        def body(t, _):
            for a in range(2):
                phi[t, a, q, pl.ds(PAD, rows)] = jnp.zeros((rows, nz), jnp.float32)
            return 0

        lax.fori_loop(0, STEPS, body, 0)

    @when(jnp.logical_not(has_l))
    def _():
        clear_halo(0)

    @when(jnp.logical_not(has_r))
    def _():
        clear_halo(planes + 1)

    for a, known in ((0, has_dn), (1, has_up)):

        @when(jnp.logical_not(known))
        def _():
            def body(p, _):
                zbuf[a, p] = jnp.zeros((half, nz), jnp.float32)
                return 0

            lax.fori_loop(0, planes, body, 0)

    count = lambda flag: jnp.where(flag, 1, 0)
    expect = 1 + count(has_dn) + count(has_up)
    expect = expect + count(has_l) * (2 - count(in_l)) + count(has_r) * (2 - count(in_r))
    pl.semaphore_wait(barrier, expect)

    for side, known, inside in ((0, has_r, in_r), (1, has_l, in_l)):

        @when(known, jnp.logical_not(inside))
        def _():
            for tgt in range(2):
                halo0(side, tgt).start()

    for i in range(len(parts)):
        for p in range(planes):
            fcopy(i, p, hi).start()
    ccopy(hi).start()

    for copy in loads:
        copy.wait()

    def send_in(a):
        for side, known, inside in ((0, has_r, in_r), (1, has_l, in_l)):

            @when(known, inside)
            def _():
                halo_in(side, a).start()

    send_in(hi)

    def scale(p, _):
        mob[p] = DT * mob[p]
        return 0

    lax.fori_loop(0, planes, scale, 0)

    def begin(k, _):
        a = lax.rem(hi + k, 2)

        @when(k == 1)
        def _():
            for i in range(len(parts)):
                for p in range(planes):
                    fcopy(i, p, other).wait_recv()
            send_in(other)

        wait_face(lambda side: halo_in(side, a), True)
        for c in range(len(chunks)):
            advance(0, a, outer, c)
            send_face(1, a, c, True)
        for c in range(len(chunks)):
            for p in inner:
                advance(0, a, p, c)
        wait_face(lambda side: halo_in(side, a), False)
        for c in range(len(chunks)):
            advance(0, a, near, c)
            send_face(1, a, c, False)
        return 0

    lax.fori_loop(0, 2, begin, 0)

    def step(t, _):
        def within(k, _):
            a = k
            for c in range(len(chunks)):
                for p in inner:
                    advance(t, a, p, c)
            return 0

        lax.fori_loop(0, 2, within, 0)

        for plane, out_side in ((outer, True), (near, False)):

            def rim(a, _):
                for c in range(len(chunks)):
                    wait_face(lambda side: halo(t, side, a, c), out_side)
                    advance(t, a, plane, c)
                    send_face(t + 1, a, c, out_side)
                return 0

            lax.fori_loop(0, 2, rim, 0)
        return 0

    lax.fori_loop(1, STEPS - 1, step, 0)

    end = STEPS - 1

    def known_z(a):
        return jnp.logical_and(img - 2 + 4 * a >= 0, img - 2 + 4 * a < images)

    def final_within(k, _):
        a = k
        for c in range(len(chunks)):
            for p in inner:
                advance(end, a, p, c)

        @when(known_z(a))
        def _():
            for p in inner:
                for c in range(2):
                    zcopy(a, p - 1, c).start()

        return 0

    lax.fori_loop(0, 2, final_within, 0)

    def final_rim(k, _):
        a = k
        for c in range(len(chunks)):
            wait_halo(end, a, c)
            advance(end, a, first, c)
            advance(end, a, last, c)

        @when(known_z(a))
        def _():
            for p in (first, last):
                for c in range(2):
                    zcopy(a, p - 1, c).start()

        return 0

    lax.fori_loop(0, 2, final_rim, 0)
    ccopy(other).wait_recv()

    def mix(a, p, c):
        at = pl.ds(pl.multiple_of(PAD + h * EXT + c * unit, 8), unit)
        mine = phi[STEPS, a, p + 1, at]
        beside = phi[STEPS, 1 - a, p + 1, at]
        along = zbuf[a, p, pl.ds(pl.multiple_of(c * unit, 8), unit)]
        f = coef[a, 0, pl.ds(0, 1)]
        side = coef[a, 1, pl.ds(0, 1)]
        use_z = jnp.broadcast_to(side, (unit, nz)) == a.astype(jnp.float32)
        return mine + f * (jnp.where(use_z, along, beside) - mine)

    def blend(u, _):
        v = lax.rem(u, 4)
        c = lax.rem(v, 2)
        p = jnp.where(u < 4, 1 + v // 2, 3 * (v // 2))
        for a, known in ((0, has_dn), (1, has_up)):

            @when(known)
            def _():
                zcopy(1 - a, p, c).wait_recv()

        xbuf[p, pl.ds(pl.multiple_of(c * unit, 8), unit)] = mix(other, p, c)
        out[0, p, pl.ds(pl.multiple_of(h * half + c * unit, 8), unit)] = mix(hi, p, c)
        xcopy(p, c, h).start()
        return 0

    lax.fori_loop(0, planes * 2, blend, 0)

    for side, known in ((0, has_r), (1, has_l)):

        @when(known)
        def _():
            for a in range(2):
                halo_in(side, a).wait_send()

            def body(i, _):
                for a in range(2):
                    for c in range(len(chunks)):
                        halo(i, side, a, c).wait_send()
                return 0

            lax.fori_loop(1, STEPS, body, 0)

    for i in range(len(parts)):
        for p in range(planes):
            fcopy(i, p, hi).wait_send()
    ccopy(hi).wait_send()

    def drain(u, _):
        p, c = u // 2, lax.rem(u, 2)
        for a, known in ((0, has_dn), (1, has_up)):

            @when(known)
            def _():
                zcopy(a, p, c).wait_send()

        xcopy(p, c, h).wait_send()
        xcopy(p, c, 1 - h).wait_recv()
        return 0

    lax.fori_loop(0, planes * 2, drain, 0)


def local(images, spaces, field, mobility, fractions, sides):
    _, planes, ny, nz = field.shape
    half = ny // 2
    dma = pltpu.SemaphoreType.DMA
    return pl.pallas_call(
        functools.partial(kernel, (images, spaces, planes, ny, nz)),
        out_shape=jax.ShapeDtypeStruct(field.shape, jnp.float32),
        in_specs=[
            pl.BlockSpec(memory_space=pltpu.HBM),
            pl.BlockSpec(memory_space=pltpu.HBM),
            pl.BlockSpec(memory_space=pltpu.SMEM),
            pl.BlockSpec(memory_space=pltpu.SMEM),
        ],
        out_specs=pl.BlockSpec(memory_space=pltpu.VMEM),
        scratch_shapes=[
            pltpu.VMEM((STEPS + 1, 2, planes + 2, half + EXT + 2 * PAD, nz), jnp.float32),
            pltpu.VMEM((planes, half + EXT, nz), jnp.float32),
            pltpu.VMEM((2, planes, half, nz), jnp.float32),
            pltpu.VMEM((planes, half, nz), jnp.float32),
            pltpu.VMEM((2, 2, 8, nz), jnp.float32),
            dma((planes + 1,)),
            dma,
            dma,
            dma((2, 2)),
            dma((2, 2)),
            dma((STEPS - 1, 2, 2, 2)),
            dma((STEPS - 1, 2, 2, 2)),
            dma((2, planes)),
            dma((2, planes)),
            dma((2, planes, 2)),
            dma((2, planes, 2)),
            dma((planes, 2)),
            dma((planes, 2)),
        ],
        compiler_params=pltpu.CompilerParams(
            collective_id=0, has_side_effects=True, vmem_limit_bytes=50 * 1024 * 1024
        ),
    )(field, mobility, fractions, sides)


def solution(mesh):
    return jax.shard_map(
        functools.partial(local, mesh.shape["image"], mesh.shape["space"]),
        mesh=mesh,
        in_specs=(P("image", "space", None, None), P("space", None, None), P("image"), P("image")),
        out_specs=P("image", "space", None, None),
        check_vma=False,
    )
```
